128 devices in a mesh: half: 4 (over y_hi, core), blk: 32 (over z, y_lo, x).
Axes of the slice: x: 4, y: 4 (y_hi: 2, y_lo: 2; y = y_hi * 2 + y_lo), z: 4, core: 2. Of those that a mesh axis runs over, the one named last changes fastest.
Arguments:
- sketch: float32 [131072, 256], P(('half', 'blk')), may hold values from -6 to 6
- near_field: float32 [131072, 64], P(('half', 'blk')), may hold values from -0.75 to 0.75
- source_one: float32 [131072, 128], P(('half', 'blk')), may hold values from -1 to 1
- source_two: float32 [131072, 128], P(('half', 'blk')), may hold values from -1 to 1
- target_one: float32 [131072, 128], P(('half', 'blk')), may hold values from -0.5 to 0.5
- target_two: float32 [131072, 128], P(('half', 'blk')), may hold values from -0.5 to 0.5
- quarter_mix: float32 [4096, 2, 128, 128], P(('half', 'blk')), may hold values from -0.375 to 0.375
- leaf_mix: float32 [4096, 2, 128, 128], P(('half', 'blk')), may hold values from -0.375 to 0.375
- target_mix_one: float32 [4096, 2, 128, 128], P(('half', 'blk')), may hold values from -0.375 to 0.375
- target_mix_two: float32 [4096, 2, 128, 128], P(('half', 'blk')), may hold values from -0.375 to 0.375
Outputs:
- product: float32 [131072, 256], P(('half', 'blk'))
The draws below stay inside these ranges and needn't reach their ends.
All inputs are finite; a program needn't handle non-finite values.
Results may differ from the reference program's by a relative error of at most 0.000061.
Values sent between devices are 32-bit elements; how exact they have to be, the bound alone decides.
A program may use at most 128 MiB of HBM per device.

```python
import jax
import jax.numpy as jnp
from jax import lax

RANK = 128
VECS = 256
GROUP = 32
LEAF = 32
ROWS = 131072
NODES = 4096


def block_scale(stream_key, extent, shards, least, largest):
    gain = 1.0
    for axis_at, parts in shards:
        steps = jax.random.uniform(jax.random.fold_in(jax.random.fold_in(stream_key, 6), axis_at), (parts,), jnp.float32, least / len(shards), largest / len(shards))
        gain = gain * jnp.repeat(jnp.exp(steps), extent[axis_at] // parts).reshape((-1,) + (1,) * (len(extent) - 1 - axis_at))
    return gain


def normal_values(key, dims, width, limit, shards=(), kind=jnp.bfloat16):
    drawn = width * jax.random.normal(key, dims, jnp.float32)
    if shards:
        drawn = drawn * block_scale(key, dims, shards, -0.22, 0.18)
    return jnp.clip(drawn, -limit, limit).astype(kind)


def setup_inputs(seed: int = 0) -> dict:
    key_of = jax.random.split(jax.random.key(seed), 11)
    sketch = normal_values(key_of[0], (ROWS, VECS), 1.0, 6.0, ((0, 128),), jnp.float32)
    near_field = normal_values(key_of[1], (ROWS, 2 * LEAF), (2 * LEAF) ** -0.5, 0.75, ((0, 128),), jnp.float32)
    source_one = normal_values(key_of[2], (ROWS, RANK), LEAF ** -0.5, 1.0, ((0, 128),), jnp.float32)
    source_two = normal_values(key_of[3], (ROWS, RANK), LEAF ** -0.5, 1.0, ((0, 128),), jnp.float32)
    target_one = normal_values(key_of[4], (ROWS, RANK), RANK ** -0.5, 0.5, ((0, 128),), jnp.float32)
    target_two = normal_values(key_of[5], (ROWS, RANK), RANK ** -0.5, 0.5, ((0, 128),), jnp.float32)
    quarter_mix = normal_values(key_of[6], (NODES, 2, RANK, RANK), (2 * RANK) ** -0.5, 0.375, ((0, 128),), jnp.float32)
    leaf_mix = normal_values(key_of[7], (NODES, 2, RANK, RANK), (2 * RANK) ** -0.5, 0.375, ((0, 128),), jnp.float32)
    target_mix_one = normal_values(key_of[8], (NODES, 2, RANK, RANK), (2 * RANK) ** -0.5, 0.375, ((0, 128),), jnp.float32)
    target_mix_two = normal_values(key_of[9], (NODES, 2, RANK, RANK), (2 * RANK) ** -0.5, 0.375, ((0, 128),), jnp.float32)
    return dict(sketch=sketch, near_field=near_field, source_one=source_one, source_two=source_two, target_one=target_one, target_two=target_two, quarter_mix=quarter_mix, leaf_mix=leaf_mix, target_mix_one=target_mix_one, target_mix_two=target_mix_two)


highest = lax.Precision.HIGHEST


def leaf_view(array, columns):
    return array.reshape(4, GROUP, GROUP, LEAF, columns)


def node_view(matrices, member):
    return matrices.reshape(4, GROUP, GROUP, 2, RANK, RANK)[:, :, :, member]


def apply_nodes(matrices, coefficients):
    return jnp.einsum('qbkst,qbktv->qbksv', matrices, coefficients, precision=highest)


def apply_back(matrices, coefficients):
    return jnp.einsum('qbkts,qbktv->qbksv', matrices, coefficients, precision=highest)


def flip_quarter(coefficients, level_bit):
    shaped = coefficients.reshape((2, 2) + coefficients.shape[1:])
    if level_bit == 1:
        shaped = shaped[::-1]
    else:
        shaped = shaped[:, ::-1]
    return shaped.reshape(coefficients.shape)


def flip_leaf(coefficients):
    shaped = coefficients.reshape(4, GROUP, GROUP // 2, 2, RANK, VECS)
    return shaped[:, :, :, ::-1].reshape(coefficients.shape)


def transport(coefficients, level_bit):
    return flip_quarter(coefficients, level_bit).transpose(0, 2, 1, 3, 4)


def compress(basis, operand):
    return jnp.einsum('qblir,qbliv->qblrv', leaf_view(basis, RANK), leaf_view(operand, VECS), precision=highest)


def expand(basis, coefficients):
    result = jnp.einsum('qblir,qblrv->qbliv', leaf_view(basis, RANK), coefficients, precision=highest)
    return result.reshape(ROWS, VECS)


def near_apply(near_field, operand, pattern):
    near_boxes = near_field.reshape(4, GROUP, GROUP // 2, 2 * LEAF, 2 * LEAF)
    blocks = operand.reshape(4, GROUP, GROUP // 2, 2 * LEAF, VECS)
    return jnp.einsum(pattern, near_boxes, blocks, precision=highest).reshape(ROWS, VECS)


def reference(sketch, near_field, source_one, source_two, target_one, target_two, quarter_mix, leaf_mix, target_mix_one, target_mix_two):
    coef_one = compress(source_one, sketch)
    mixed_one = apply_nodes(node_view(quarter_mix, 0), coef_one) + apply_nodes(node_view(quarter_mix, 1), flip_quarter(coef_one, 0))
    arrived_one = transport(mixed_one, 1)
    out_one = apply_nodes(node_view(target_mix_one, 0), arrived_one) + apply_nodes(node_view(target_mix_one, 1), flip_leaf(arrived_one))
    coef_two = compress(source_two, sketch)
    mixed_two = apply_nodes(node_view(leaf_mix, 0), coef_two) + apply_nodes(node_view(leaf_mix, 1), flip_leaf(coef_two))
    arrived_two = transport(mixed_two, 0)
    out_two = apply_nodes(node_view(target_mix_two, 0), arrived_two) + apply_nodes(node_view(target_mix_two, 1), flip_leaf(arrived_two))
    sketched = 0.5 * sketch + near_apply(near_field, sketch, 'qbkij,qbkjv->qbkiv') + expand(target_one, out_one) + expand(target_two, out_two)

    head_one = compress(target_one, sketched)
    back_one = apply_back(node_view(target_mix_one, 0), head_one) + flip_leaf(apply_back(node_view(target_mix_one, 1), head_one))
    landed_one = transport(back_one, 1)
    tail_one = apply_back(node_view(quarter_mix, 0), landed_one) + flip_quarter(apply_back(node_view(quarter_mix, 1), landed_one), 0)
    head_two = compress(target_two, sketched)
    back_two = apply_back(node_view(target_mix_two, 0), head_two) + flip_leaf(apply_back(node_view(target_mix_two, 1), head_two))
    landed_two = transport(back_two, 0)
    tail_two = apply_back(node_view(leaf_mix, 0), landed_two) + flip_leaf(apply_back(node_view(leaf_mix, 1), landed_two))
    product = 0.5 * sketched + near_apply(near_field, sketched, 'qbkji,qbkjv->qbkiv') + expand(source_one, tail_one) + expand(source_two, tail_two)
    return product
```

```python
import functools

import jax
import jax.numpy as jnp
from jax import lax
from jax.experimental import pallas as pl
from jax.experimental.pallas import tpu as pltpu
from jax.sharding import PartitionSpec as P

MESH = pl.DeviceIdType.MESH
HIGH = lax.Precision.HIGHEST
F32 = jnp.float32


def dot(a, b):
    return lax.dot_general(a, b, (((1,), (0,)), ((), ())), precision=HIGH, preferred_element_type=F32)


def dot_nt(a, b):
    return lax.dot_general(a, b, (((1,), (1,)), ((), ())), precision=HIGH, preferred_element_type=F32)


def dot_tn(a, b):
    return lax.dot_general(a, b, (((0,), (0,)), ((), ())), precision=HIGH, preferred_element_type=F32)


def xor(a, b, bits):
    total = 0
    for k in range(bits):
        w = 1 << k
        total = total + lax.rem(lax.div(a, w) + lax.div(b, w), 2) * w
    return total


def reversed_bits(a, bits):
    total = 0
    for k in range(bits):
        total = total + lax.rem(lax.div(a, 1 << k), 2) * (1 << (bits - 1 - k))
    return total


def rows(ref, start, count):
    return ref.at[pl.ds(pl.multiple_of(start, 32), count)]


def kernel(
    groups,
    sketch,
    near,
    source_one,
    source_two,
    target_one,
    target_two,
    quarter_mix,
    leaf_mix,
    target_mix_one,
    target_mix_two,
    product,
    v_own,
    near_own,
    s_one,
    s_one_peer,
    s_two,
    t_one,
    t_two,
    qm,
    lm,
    tm_one,
    tm_two,
    a_send,
    b_send,
    a_recv,
    b_recv,
    vf,
    vc,
    p_one,
    p_two,
    yf,
    yx,
    yc,
    yf_recv,
    yc_recv,
    load_sem,
    mix_sem,
    peer_sem,
    send_sem,
    vf_sem,
    vp_sem,
    vc_sem,
    a_sem,
    b_sem,
    x_sem,
    yf_sem,
    yc_sem,
):
    pairs = groups // 2
    bits = pairs.bit_length() - 1
    q = lax.axis_index("half")
    m = lax.axis_index("blk")
    mine = lax.div(m, 2)
    q_peer = xor(q, 1, 2)
    q_far = xor(q, 2, 2)

    def pair_at(step):
        return xor(mine, reversed_bits(step, bits), bits)

    barrier = pltpu.get_barrier_semaphore()

    def greet(n, carry):
        pl.semaphore_signal(barrier, inc=1, device_id=(q_far, n), device_id_type=MESH)
        pl.semaphore_signal(barrier, inc=1, device_id=(q_peer, n), device_id_type=MESH)
        return carry

    lax.fori_loop(0, groups, greet, 0)

    loads = [
        pltpu.make_async_copy(src, dst, load_sem.at[k])
        for k, (src, dst) in enumerate(
            (
                (sketch, v_own),
                (source_one, s_one),
                (source_two, s_two),
                (target_one, t_one),
                (target_two, t_two),
                (near, near_own),
            )
        )
    ]
    for copy in loads:
        copy.start()

    def mix_copy(k, p):
        src, dst = ((quarter_mix, qm), (leaf_mix, lm), (target_mix_one, tm_one), (target_mix_two, tm_two))[k]
        here = pl.ds(2 * p, 2)
        return pltpu.make_async_copy(src.at[here], dst.at[here], mix_sem.at[k, p])

    def load_source_mix(step, carry):
        p = pair_at(step)
        mix_copy(0, p).start()
        mix_copy(1, p).start()
        return carry

    def load_target_mix(step, carry):
        p = pair_at(step)
        mix_copy(2, p).start()
        mix_copy(3, p).start()
        return carry

    lax.fori_loop(0, pairs, load_source_mix, 0)
    lax.fori_loop(0, pairs, load_target_mix, 0)

    def remote(src, dst, k, recv, to):
        return pltpu.make_async_remote_copy(
            src_ref=src, dst_ref=dst, send_sem=send_sem.at[k], recv_sem=recv, device_id=to, device_id_type=MESH
        )

    def vf_copy(n):
        return remote(rows(v_own, 32 * n, 32), rows(vf, 64 * m, 32), 0, vf_sem.at[m], (q_far, n))

    def vc_copy(p, n):
        return remote(rows(v_own, 64 * p, 64), rows(vc, 64 * m, 64), 1, vc_sem.at[m], (q_peer, n))

    def a_copy(n):
        return remote(rows(a_send, 64 * n, 64), rows(a_recv, 64 * m, 64), 2, a_sem.at[m], (q_far, n))

    def b_copy(n):
        return remote(rows(b_send, 64 * n, 64), rows(b_recv, 64 * m, 64), 3, b_sem.at[m], (q_peer, n))

    def vp_copy(b):
        return remote(rows(vf, 64 * b, 32), rows(vf, 64 * b + 32, 32), 4, vp_sem.at[b], (q_peer, m))

    def x_copy(b):
        return remote(rows(yf, 64 * b + 32, 32), rows(yx, 32 * b, 32), 5, x_sem.at[b], (q_peer, m))

    def yf_copy(b):
        return remote(rows(yf, 64 * b, 32), rows(yf_recv, 32 * m, 32), 6, yf_sem.at[m], (q_far, b))

    def yc_copy(b):
        return remote(rows(yc, 64 * b, 64), rows(yc_recv, 64 * m, 64), 7, yc_sem.at[m], (q_peer, b))

    peer_copy = remote(s_one, s_one_peer, 8, peer_sem, (q_peer, m))

    loads[0].wait()
    loads[1].wait()
    pl.semaphore_wait(barrier, 2 * groups)
    peer_copy.start()

    def send_vectors(step, carry):
        p = pair_at(step)
        for n in (2 * p, 2 * p + 1):
            vf_copy(n).start()
            vc_copy(p, n).start()
        return carry

    lax.fori_loop(0, pairs, send_vectors, 0)
    loads[2].wait()
    peer_copy.wait()

    def send_sources(step, carry):
        p = pair_at(step)
        mix_copy(0, p).wait()
        mix_copy(1, p).wait()
        low, high = 2 * p, 2 * p + 1
        first = [rows(s_two, 32 * low, 32)[...], rows(s_two, 32 * high, 32)[...]]
        for k, n in enumerate((low, high)):
            rows(b_send, 64 * n, 32)[...] = dot_nt(first[0], lm[n, k])
            rows(b_send, 64 * n + 32, 32)[...] = dot_nt(first[1], lm[n, 1 - k])
            rows(a_send, 64 * n, 32)[...] = dot_nt(rows(s_one, 32 * n, 32)[...], qm[n, 0])
            rows(a_send, 64 * n + 32, 32)[...] = dot_nt(rows(s_one_peer, 32 * n, 32)[...], qm[n, 1])
        for n in (low, high):
            a_copy(n).start()
            b_copy(n).start()
        return carry

    lax.fori_loop(0, pairs, send_sources, 0)
    loads[3].wait()
    loads[4].wait()
    loads[5].wait()

    def make_targets(step, carry):
        p = pair_at(step)
        mix_copy(2, p).wait()
        mix_copy(3, p).wait()
        low, high = 2 * p, 2 * p + 1
        for basis, mix, out in ((t_one, tm_one, p_one), (t_two, tm_two, p_two)):
            for k, n in enumerate((low, high)):
                t = rows(basis, 32 * n, 32)[...]
                rows(out, 128 * p + 32 * k, 32)[...] = dot(t, mix[n, k])
                rows(out, 128 * p + 64 + 32 * k, 32)[...] = dot(t, mix[n, 1 - k])
        return carry

    lax.fori_loop(0, pairs, make_targets, 0)

    def forward(p):
        for b in (2 * p, 2 * p + 1):
            vf_copy_in = vp_copy(b)
            remote(rows(v_own, 0, 32), rows(vf, 64 * b, 32), 0, vf_sem.at[b], (q_far, m)).wait_recv()
            vf_copy_in.start()

    def apply(p):
        low, high = 2 * p, 2 * p + 1
        for b in (low, high):
            remote(rows(vf, 64 * b, 32), rows(vf, 64 * b + 32, 32), 4, vp_sem.at[b], (q_peer, m)).wait_recv()
            remote(rows(v_own, 0, 64), rows(vc, 64 * b, 64), 1, vc_sem.at[b], (q_peer, m)).wait_recv()
            remote(rows(a_send, 0, 64), rows(a_recv, 64 * b, 64), 2, a_sem.at[b], (q_far, m)).wait_recv()
            remote(rows(b_send, 0, 64), rows(b_recv, 64 * b, 64), 3, b_sem.at[b], (q_peer, m)).wait_recv()
        v = rows(v_own, 64 * p, 64)[...]
        box = rows(near_own, 64 * p, 64)[...]
        w = 0.5 * v + dot(box, v)
        for k, b in enumerate((low, high)):
            f = rows(p_one, 128 * p + 64 * k, 64)[...]
            c = rows(p_two, 128 * p + 64 * k, 64)[...]
            w = w + dot(dot_nt(f, rows(a_recv, 64 * b, 64)[...]), rows(vf, 64 * b, 64)[...])
            w = w + dot(dot_nt(c, rows(b_recv, 64 * b, 64)[...]), rows(vc, 64 * b, 64)[...])
        for k, b in enumerate((low, high)):
            f = rows(p_one, 128 * p + 64 * k, 64)[...]
            c = rows(p_two, 128 * p + 64 * k, 64)[...]
            rows(yf, 64 * b, 64)[...] = dot(dot_nt(rows(a_recv, 64 * b, 64)[...], f), w)
            rows(yc, 64 * b, 64)[...] = dot(dot_nt(rows(b_recv, 64 * b, 64)[...], c), w)
        rows(product, 64 * p, 64)[...] = 0.5 * w + dot_tn(box, w)
        for b in (low, high):
            x_copy(b).start()
            yc_copy(b).start()


    def join(p):
        for b in (2 * p, 2 * p + 1):
            remote(rows(yf, 0, 32), rows(yx, 32 * b, 32), 5, x_sem.at[b], (q_peer, m)).wait_recv()
            rows(yf, 64 * b, 32)[...] += rows(yx, 32 * b, 32)[...]
        for b in (2 * p, 2 * p + 1):
            yf_copy(b).start()

    def stream(step, carry):
        @pl.when(step < pairs)
        def _():
            forward(pair_at(step))

        @pl.when((step >= 1) & (step < pairs + 1))
        def _():
            apply(pair_at(step - 1))

        @pl.when(step >= 2)
        def _():
            join(pair_at(step - 2))

        return carry

    lax.fori_loop(0, pairs + 2, stream, 0)

    def finish(step, carry):
        p = pair_at(step)
        low, high = 2 * p, 2 * p + 1
        for b in (low, high):
            remote(rows(yf, 0, 32), rows(yf_recv, 32 * b, 32), 6, yf_sem.at[b], (q_far, m)).wait_recv()
            remote(rows(yc, 0, 64), rows(yc_recv, 64 * b, 64), 7, yc_sem.at[b], (q_peer, m)).wait_recv()
        here = rows(product, 64 * p, 64)
        here[...] = (
            here[...]
            + rows(yf_recv, 64 * p, 64)[...]
            + (rows(yc_recv, 128 * p, 64)[...] + rows(yc_recv, 128 * p + 64, 64)[...])
        )
        return carry

    lax.fori_loop(0, pairs, finish, 0)

    for k, ref in (
        (0, v_own),
        (1, vc),
        (2, a_send),
        (3, b_send),
        (4, v_own),
        (5, v_own),
        (6, v_own),
        (7, vc),
    ):
        remote(ref, ref, k, peer_sem, (q_peer, m)).wait_send()


def body(sketch, near_field, source_one, source_two, target_one, target_two, quarter_mix, leaf_mix, mix_one, mix_two):
    groups = lax.axis_size("blk")
    local, vectors = sketch.shape
    rank = source_one.shape[1]
    any_space = pl.BlockSpec(memory_space=pl.ANY)
    basis = pltpu.VMEM((local, rank), F32)
    mixes = pltpu.VMEM(quarter_mix.shape, F32)
    single = pltpu.VMEM((local, vectors), F32)
    double = pltpu.VMEM((2 * local, vectors), F32)
    nodes = pltpu.VMEM((2 * local, rank), F32)
    dma = pltpu.SemaphoreType.DMA


    return pl.pallas_call(
        functools.partial(kernel, groups),
        out_shape=jax.ShapeDtypeStruct((local, vectors), F32),
        in_specs=[any_space] * 10,
        out_specs=pl.BlockSpec(memory_space=pltpu.VMEM),
        scratch_shapes=[
            single,
            pltpu.VMEM(near_field.shape, F32),
            basis,
            basis,
            basis,
            basis,
            basis,
            mixes,
            mixes,
            mixes,
            mixes,
            nodes,
            nodes,
            nodes,
            nodes,
            double,
            double,
            nodes,
            nodes,
            double,
            single,
            double,
            single,
            double,
            dma((6,)),
            dma((4, groups // 2)),
            dma(()),
            dma((9,)),
            dma((groups,)),
            dma((groups,)),
            dma((groups,)),
            dma((groups,)),
            dma((groups,)),
            dma((groups,)),
            dma((groups,)),
            dma((groups,)),
        ],
        compiler_params=pltpu.CompilerParams(
            collective_id=0, has_side_effects=True, vmem_limit_bytes=60 * 1024 * 1024
        ),
    )(sketch, near_field, source_one, source_two, target_one, target_two, quarter_mix, leaf_mix, mix_one, mix_two)


def solution(mesh):
    rows_split = P(("half", "blk"), None)
    nodes_split = P(("half", "blk"), None, None, None)
    return jax.shard_map(
        body,
        mesh=mesh,
        in_specs=(rows_split,) * 6 + (nodes_split,) * 4,
        out_specs=rows_split,
        check_vma=False,
    )
```

```python
import functools

import jax
import jax.numpy as jnp
from jax import lax
from jax.experimental import pallas as pl
from jax.experimental.pallas import tpu as pltpu
from jax.sharding import PartitionSpec as P

MESH = pl.DeviceIdType.MESH
HIGH = lax.Precision.HIGHEST
F32 = jnp.float32


def dot(a, b):
    return lax.dot_general(a, b, (((1,), (0,)), ((), ())), precision=HIGH, preferred_element_type=F32)


def dot_nt(a, b):
    return lax.dot_general(a, b, (((1,), (1,)), ((), ())), precision=HIGH, preferred_element_type=F32)


def dot_tn(a, b):
    return lax.dot_general(a, b, (((0,), (0,)), ((), ())), precision=HIGH, preferred_element_type=F32)


def xor(a, b, bits):
    total = 0
    for k in range(bits):
        w = 1 << k
        total = total + lax.rem(lax.div(a, w) + lax.div(b, w), 2) * w
    return total


def reversed_bits(a, bits):
    total = 0
    for k in range(bits):
        total = total + lax.rem(lax.div(a, 1 << k), 2) * (1 << (bits - 1 - k))
    return total


RELAYED = dict(relay=1, cross=2, share=3, target=3, apply=4, join=5, add=6, gather=7)
STRAIGHT = dict(relay=1, share=1, target=1, apply=2, join=3, gather=4)
AHEAD = 2


def rows(ref, start, count):
    return ref.at[pl.ds(pl.multiple_of(start, 32), count)]


def kernel(
    groups,
    sketch,
    near,
    source_one,
    source_two,
    target_one,
    target_two,
    quarter_mix,
    leaf_mix,
    target_mix_one,
    target_mix_two,
    product,
    v_own,
    near_own,
    s_one,
    s_one_peer,
    s_two,
    t_one,
    t_two,
    qm,
    lm,
    tm_one,
    tm_two,
    a_send,
    b_send,
    a_recv,
    b_recv,
    vf,
    vc,
    p_one,
    p_two,
    yf,
    yx,
    yc,
    yn,
    yr,
    yf_recv,
    yc_recv,
    load_sem,
    mix_sem,
    peer_sem,
    send_sem,
    vf_sem,
    vp_sem,
    vc_sem,
    vn_sem,
    a_sem,
    b_sem,
    x_sem,
    yn_sem,
    yr_sem,
    yf_sem,
    yc_sem,
):
    pairs = groups // 2
    half = pairs // 2
    bits = pairs.bit_length() - 1
    q = lax.axis_index("half")
    m = lax.axis_index("blk")
    mine = lax.div(m, 2)
    q_peer = xor(q, 1, 2)
    q_far = xor(q, 2, 2)
    beside = xor(m, 1, 1) + 2 * mine

    def pair_at(step):
        inner = reversed_bits(lax.rem(step, half), bits - 1)
        return xor(mine, inner + inner - lax.rem(inner, 2) + 2 * lax.div(step, half), bits)

    def direct_at(step):
        return lax.div(step, half) * 32

    def entry(p):
        return lax.rem(m + mine + p, 2)

    barrier = pltpu.get_barrier_semaphore()

    def greet(n, carry):
        pl.semaphore_signal(barrier, inc=1, device_id=(q_far, n), device_id_type=MESH)
        pl.semaphore_signal(barrier, inc=1, device_id=(q_peer, n), device_id_type=MESH)
        return carry

    lax.fori_loop(0, groups, greet, 0)
    pl.semaphore_signal(barrier, inc=1, device_id=(q, beside), device_id_type=MESH)

    loads = [
        pltpu.make_async_copy(src, dst, load_sem.at[k])
        for k, (src, dst) in enumerate(
            (
                (sketch, v_own),
                (source_one, s_one),
                (source_two, s_two),
                (target_one, t_one),
                (target_two, t_two),
                (near, near_own),
            )
        )
    ]
    for copy in loads:
        copy.start()

    def mix_copy(k, p):
        src, dst = ((quarter_mix, qm), (leaf_mix, lm), (target_mix_one, tm_one), (target_mix_two, tm_two))[k]
        here = pl.ds(2 * p, 2)
        return pltpu.make_async_copy(src.at[here], dst.at[here], mix_sem.at[k, p])

    def load_source_mix(step, carry):
        p = pair_at(step)
        mix_copy(0, p).start()
        mix_copy(1, p).start()
        return carry

    def load_target_mix(step, carry):
        p = pair_at(step)
        mix_copy(2, p).start()
        mix_copy(3, p).start()
        return carry

    lax.fori_loop(0, pairs, load_source_mix, 0)
    lax.fori_loop(0, pairs, load_target_mix, 0)

    def remote(src, dst, k, recv, to):
        return pltpu.make_async_remote_copy(
            src_ref=src, dst_ref=dst, send_sem=send_sem.at[k], recv_sem=recv, device_id=to, device_id_type=MESH
        )

    def vf_copy(n):
        return remote(rows(v_own, 32 * n, 32), rows(vf, 64 * m, 32), 0, vf_sem.at[m], (q_far, n))

    def vc_copy(p):
        n = 2 * p + entry(p)
        return remote(rows(v_own, 64 * p, 64), rows(vc, 64 * m, 64), 1, vc_sem.at[m], (q_peer, n))

    def vn_copy(b):
        return remote(rows(vc, 64 * b, 64), rows(vc, 64 * b, 64), 9, vn_sem.at[b], (q, beside))

    def yn_copy(p, b):
        return remote(rows(yc, 64 * b, 64), rows(yn, 64 * p, 64), 10, yn_sem.at[p], (q, beside))

    def a_copy(n):
        return remote(rows(a_send, 64 * n, 64), rows(a_recv, 64 * m, 64), 2, a_sem.at[m], (q_far, n))

    def b_copy(n):
        return remote(rows(b_send, 64 * n, 64), rows(b_recv, 64 * m, 64), 3, b_sem.at[m], (q_peer, n))

    def vr_copy(b):
        return remote(rows(vc, 64 * b + 32 * lax.rem(m, 2), 32), rows(vf, 64 * b + 32, 32), 11, vf_sem.at[b], (q_far, m))

    def vp_copy(b, off):
        return remote(rows(vf, 64 * b + 32 - off, 32), rows(vf, 64 * b + off, 32), 4, vp_sem.at[b], (q_peer, m))

    def x_copy(b, off):
        return remote(rows(yf, 64 * b + off, 32), rows(yx, 32 * b, 32), 5, x_sem.at[b], (q_peer, m))

    def yr_copy(b):
        return remote(rows(yf, 64 * b + 32, 32), rows(yr, 32 * b, 32), 12, yr_sem.at[b], (q_far, m))

    def yf_copy(b):
        return remote(rows(yf, 64 * b, 32), rows(yf_recv, 32 * m, 32), 6, yf_sem.at[m], (q_far, b))

    def yc_copy(b):
        return remote(rows(yc, 64 * b, 64), rows(yc_recv, 64 * mine, 64), 7, yc_sem.at[mine], (q_peer, b))

    peer_copy = remote(s_one, s_one_peer, 8, peer_sem, (q_peer, m))

    loads[0].wait()
    loads[1].wait()
    pl.semaphore_wait(barrier, 2 * groups + 1)
    peer_copy.start()

    def both(p):
        return (2 * p, 2 * p + 1)

    def arrived(dst, sem):
        remote(dst, dst, 0, sem, (q_peer, m)).wait_recv()

    def send_vectors(step):
        p = pair_at(step)
        vc_copy(p).start()

        @pl.when(step >= half)
        def _():
            for n in both(p):
                vf_copy(n).start()

    def make_sources(step):
        p = pair_at(step)
        mix_copy(0, p).wait()
        mix_copy(1, p).wait()
        first = [rows(s_two, 32 * n, 32)[...] for n in both(p)]
        for k, n in enumerate(both(p)):
            rows(b_send, 64 * n, 32)[...] = dot_nt(first[0], lm[n, k])
            rows(b_send, 64 * n + 32, 32)[...] = dot_nt(first[1], lm[n, 1 - k])
            rows(a_send, 64 * n, 32)[...] = dot_nt(rows(s_one, 32 * n, 32)[...], qm[n, 0])
            rows(a_send, 64 * n + 32, 32)[...] = dot_nt(rows(s_one_peer, 32 * n, 32)[...], qm[n, 1])

    def send_sources(step):
        for n in both(pair_at(step)):
            a_copy(n).start()
            b_copy(n).start()

    def make_targets(step):
        p = pair_at(step)
        mix_copy(2, p).wait()
        mix_copy(3, p).wait()
        for basis, mix, out in ((t_one, tm_one, p_one), (t_two, tm_two, p_two)):
            for k, n in enumerate(both(p)):
                t = rows(basis, 32 * n, 32)[...]
                rows(out, 128 * p + 32 * k, 32)[...] = dot(t, mix[n, k])
                rows(out, 128 * p + 64 + 32 * k, 32)[...] = dot(t, mix[n, 1 - k])

    def relay(step):
        p = pair_at(step)
        b = 2 * p + entry(p)
        arrived(rows(vc, 64 * b, 64), vc_sem.at[b])
        vn_copy(b).start()

        @pl.when(step < half)
        def _():
            vr_copy(b).start()

    def cross(step):
        p = pair_at(step)
        b = 2 * p + 1 - entry(p)
        arrived(rows(vc, 64 * b, 64), vn_sem.at[b])
        vr_copy(b).start()

    def share(step):
        off = direct_at(step)
        for b in both(pair_at(step)):
            arrived(rows(vf, 64 * b + 32 - off, 32), vf_sem.at[b])
            vp_copy(b, off).start()

    def apply(step):
        p = pair_at(step)
        off = direct_at(step)
        for b in both(p):
            arrived(rows(vf, 64 * b + off, 32), vp_sem.at[b])
            arrived(rows(a_recv, 64 * b, 64), a_sem.at[b])
            arrived(rows(b_recv, 64 * b, 64), b_sem.at[b])
        @pl.when(step >= half)
        def _():
            b = 2 * p + 1 - entry(p)
            arrived(rows(vc, 64 * b, 64), vn_sem.at[b])

        v = rows(v_own, 64 * p, 64)[...]
        box = rows(near_own, 64 * p, 64)[...]
        w = 0.5 * v + dot(box, v)
        for k, b in enumerate(both(p)):
            f = rows(p_one, 128 * p + 64 * k, 64)[...]
            c = rows(p_two, 128 * p + 64 * k, 64)[...]
            w = w + dot(dot_nt(f, rows(a_recv, 64 * b, 64)[...]), rows(vf, 64 * b, 64)[...])
            w = w + dot(dot_nt(c, rows(b_recv, 64 * b, 64)[...]), rows(vc, 64 * b, 64)[...])
        for k, b in enumerate(both(p)):
            f = rows(p_one, 128 * p + 64 * k, 64)[...]
            c = rows(p_two, 128 * p + 64 * k, 64)[...]
            rows(yf, 64 * b, 64)[...] = dot(dot_nt(rows(a_recv, 64 * b, 64)[...], f), w)
            rows(yc, 64 * b, 64)[...] = dot(dot_nt(rows(b_recv, 64 * b, 64)[...], c), w)
        rows(product, 64 * p, 64)[...] = 0.5 * w + dot_tn(box, w)

    def send_applied(step):
        p = pair_at(step)
        off = direct_at(step)
        for b in both(p):
            x_copy(b, off).start()

        @pl.when(step >= half)
        def _():
            yn_copy(p, 2 * p + 1 - entry(p)).start()

    def join(step):
        off = direct_at(step)
        for b in both(pair_at(step)):
            arrived(rows(yx, 32 * b, 32), x_sem.at[b])
            rows(yf, 64 * b + 32 - off, 32)[...] += rows(yx, 32 * b, 32)[...]

    def send_joined(step):
        p = pair_at(step)

        @pl.when(step < half)
        def _():
            for b in both(p):
                yr_copy(b).start()

        @pl.when(step >= half)
        def _():
            for b in both(p):
                yf_copy(b).start()

    def add(step):
        for b in both(pair_at(step)):
            arrived(rows(yr, 32 * b, 32), yr_sem.at[b])
            rows(yc, 64 * b + 32 * lax.rem(m, 2), 32)[...] += rows(yr, 32 * b, 32)[...]

    def send_added(step):
        p = pair_at(step)
        yn_copy(p, 2 * p + 1 - entry(p)).start()

    def gather(step):
        p = pair_at(step)
        b = 2 * p + entry(p)
        arrived(rows(yn, 64 * p, 64), yn_sem.at[p])
        rows(yc, 64 * b, 64)[...] += rows(yn, 64 * p, 64)[...]

    def send_gathered(step):
        p = pair_at(step)
        yc_copy(2 * p + entry(p)).start()

    def staged(step, stage, lag, first, last):
        @pl.when((step >= first + lag) & (step < last + lag))
        def _():
            stage(step - lag)

    def staggered(step, name, *stages):
        for stage in stages:
            if name in RELAYED:
                staged(step, stage, RELAYED[name], 0, half)
            if name in STRAIGHT:
                staged(step, stage, STRAIGHT[name], half, pairs)

    for step in range(AHEAD):
        send_vectors(step)
    for copy in loads[2:]:
        copy.wait()
    peer_copy.wait()

    def stream(step, carry):
        @pl.when(step < pairs - AHEAD)
        def _():
            send_vectors(step + AHEAD)

        staged(step, make_sources, 0, 0, pairs)
        staggered(step, "relay", relay)
        staggered(step, "cross", cross)
        staggered(step, "share", share)
        staged(step, send_sources, 0, 0, pairs)
        staggered(step, "gather", gather)
        staggered(step, "add", add)
        staggered(step, "join", join)
        staggered(step, "gather", send_gathered)
        staggered(step, "add", send_added)
        staggered(step, "join", send_joined)
        staggered(step, "target", make_targets)
        staggered(step, "apply", apply)
        staggered(step, "apply", send_applied)
        return carry

    lax.fori_loop(0, half + max(RELAYED["gather"], half + STRAIGHT["gather"]), stream, 0)

    def finish(step, carry):
        p = pair_at(step)
        arrived(rows(yc_recv, 64 * p, 64), yc_sem.at[p])
        rows(product, 64 * p, 64)[...] += rows(yc_recv, 64 * p, 64)[...]

        @pl.when(step >= half)
        def _():
            for b in both(p):
                arrived(rows(yf_recv, 32 * b, 32), yf_sem.at[b])
            rows(product, 64 * p, 64)[...] += rows(yf_recv, 64 * p, 64)[...]

        return carry

    lax.fori_loop(0, pairs, finish, 0)

    whole, part = v_own, rows(v_own, 0, 16 * groups)
    for k, ref in (
        (0, part),
        (1, whole),
        (2, a_send),
        (3, b_send),
        (4, whole),
        (5, whole),
        (6, part),
        (7, whole),
        (9, whole),
        (10, whole),
        (11, part),
        (12, part),
    ):
        remote(ref, ref, k, peer_sem, (q_peer, m)).wait_send()


def body(sketch, near_field, source_one, source_two, target_one, target_two, quarter_mix, leaf_mix, mix_one, mix_two):
    groups = lax.axis_size("blk")
    local, vectors = sketch.shape
    rank = source_one.shape[1]
    any_space = pl.BlockSpec(memory_space=pl.ANY)
    basis = pltpu.VMEM((local, rank), F32)
    mixes = pltpu.VMEM(quarter_mix.shape, F32)
    single = pltpu.VMEM((local, vectors), F32)
    double = pltpu.VMEM((2 * local, vectors), F32)
    nodes = pltpu.VMEM((2 * local, rank), F32)
    dma = pltpu.SemaphoreType.DMA


    return pl.pallas_call(
        functools.partial(kernel, groups),
        out_shape=jax.ShapeDtypeStruct((local, vectors), F32),
        in_specs=[any_space] * 10,
        out_specs=pl.BlockSpec(memory_space=pltpu.VMEM),
        scratch_shapes=[
            single,
            pltpu.VMEM(near_field.shape, F32),
            basis,
            basis,
            basis,
            basis,
            basis,
            mixes,
            mixes,
            mixes,
            mixes,
            nodes,
            nodes,
            nodes,
            nodes,
            double,
            double,
            nodes,
            nodes,
            double,
            single,
            double,
            single,
            single,
            single,
            single,
            dma((6,)),
            dma((4, groups // 2)),
            dma(()),
            dma((13,)),
            dma((groups,)),
            dma((groups,)),
            dma((groups,)),
            dma((groups,)),
            dma((groups,)),
            dma((groups,)),
            dma((groups,)),
            dma((groups // 2,)),
            dma((groups,)),
            dma((groups,)),
            dma((groups // 2,)),
        ],
        compiler_params=pltpu.CompilerParams(
            collective_id=0, has_side_effects=True, vmem_limit_bytes=60 * 1024 * 1024
        ),
    )(sketch, near_field, source_one, source_two, target_one, target_two, quarter_mix, leaf_mix, mix_one, mix_two)


def solution(mesh):
    rows_split = P(("half", "blk"), None)
    nodes_split = P(("half", "blk"), None, None, None)
    return jax.shard_map(
        body,
        mesh=mesh,
        in_specs=(rows_split,) * 6 + (nodes_split,) * 4,
        out_specs=rows_split,
        check_vma=False,
    )
```

```python
import functools

import jax
import jax.numpy as jnp
from jax import lax
from jax.experimental import pallas as pl
from jax.experimental.pallas import tpu as pltpu
from jax.sharding import PartitionSpec as P

MESH = pl.DeviceIdType.MESH
HIGH = lax.Precision.HIGHEST
F32 = jnp.float32


def dot(a, b):
    return lax.dot_general(a, b, (((1,), (0,)), ((), ())), precision=HIGH, preferred_element_type=F32)


def dot_nt(a, b):
    return lax.dot_general(a, b, (((1,), (1,)), ((), ())), precision=HIGH, preferred_element_type=F32)


def dot_tn(a, b):
    return lax.dot_general(a, b, (((0,), (0,)), ((), ())), precision=HIGH, preferred_element_type=F32)


def xor(a, b, bits):
    total = 0
    for k in range(bits):
        w = 1 << k
        total = total + lax.rem(lax.div(a, w) + lax.div(b, w), 2) * w
    return total


def reversed_bits(a, bits):
    total = 0
    for k in range(bits):
        total = total + lax.rem(lax.div(a, 1 << k), 2) * (1 << (bits - 1 - k))
    return total


RELAYED = dict(relay=1, cross=2, share=3, target=3, apply=4, join=5, add=6, gather=7)
STRAIGHT = dict(relay=1, share=1, target=1, apply=2, join=3, gather=4)
AHEAD = 2


def rows(ref, start, count):
    return ref.at[pl.ds(pl.multiple_of(start, 32), count)]


def kernel(
    groups,
    sketch,
    near,
    source_one,
    source_two,
    target_one,
    target_two,
    quarter_mix,
    leaf_mix,
    target_mix_one,
    target_mix_two,
    product,
    v_own,
    near_flat,
    near_own,
    s_one,
    s_one_peer,
    s_two,
    t_one,
    t_two,
    qm,
    lm,
    tm_one,
    tm_two,
    a_send,
    b_send,
    a_recv,
    b_recv,
    vf,
    vc,
    p_one,
    p_two,
    yf,
    yx,
    yc,
    yn,
    yr,
    yf_recv,
    yc_recv,
    load_sem,
    mix_sem,
    peer_sem,
    send_sem,
    vf_sem,
    vp_sem,
    vc_sem,
    vn_sem,
    a_sem,
    b_sem,
    x_sem,
    yn_sem,
    yr_sem,
    yf_sem,
    yc_sem,
):
    pairs = groups // 2
    half = pairs // 2
    bits = pairs.bit_length() - 1
    q = lax.axis_index("half")
    m = lax.axis_index("blk")
    mine = lax.div(m, 2)
    q_peer = xor(q, 1, 2)
    q_far = xor(q, 2, 2)
    beside = xor(m, 1, 1) + 2 * mine

    def pair_at(step):
        inner = reversed_bits(lax.rem(step, half), bits - 1)
        inner = inner + lax.div(step, half) * (half - 1 - 2 * inner)
        return xor(mine, inner + inner - lax.rem(inner, 2) + 2 * lax.div(step, half), bits)

    def direct_at(step):
        return lax.div(step, half) * 32

    def entry(p):
        return lax.rem(m + mine + p, 2)

    barrier = pltpu.get_barrier_semaphore()

    def greet(n, carry):
        pl.semaphore_signal(barrier, inc=1, device_id=(q_far, n), device_id_type=MESH)
        pl.semaphore_signal(barrier, inc=1, device_id=(q_peer, n), device_id_type=MESH)
        return carry

    lax.fori_loop(0, groups, greet, 0)
    pl.semaphore_signal(barrier, inc=1, device_id=(q, beside), device_id_type=MESH)

    loads = [
        pltpu.make_async_copy(src, dst, load_sem.at[k])
        for k, (src, dst) in enumerate(
            (
                (sketch, v_own),
                (source_one, s_one),
                (source_two, s_two),
                (target_one, t_one),
                (target_two, t_two),
                (near, near_flat),
            )
        )
    ]
    for copy in loads:
        copy.start()

    def mix_copy(k, p):
        src, dst = ((quarter_mix, qm), (leaf_mix, lm), (target_mix_one, tm_one), (target_mix_two, tm_two))[k]
        here = pl.ds(2 * p, 2)
        return pltpu.make_async_copy(src.at[here], dst.at[here], mix_sem.at[k, p])

    def load_source_mix(step, carry):
        p = pair_at(step)
        mix_copy(0, p).start()
        mix_copy(1, p).start()
        return carry

    def load_target_mix(step, carry):
        p = pair_at(step)
        mix_copy(2, p).start()
        mix_copy(3, p).start()
        return carry

    lax.fori_loop(0, pairs, load_source_mix, 0)
    lax.fori_loop(0, pairs, load_target_mix, 0)

    def remote(src, dst, k, recv, to):
        return pltpu.make_async_remote_copy(
            src_ref=src, dst_ref=dst, send_sem=send_sem.at[k], recv_sem=recv, device_id=to, device_id_type=MESH
        )

    def vf_copy(n):
        return remote(rows(v_own, 32 * n, 32), rows(vf, 64 * m, 32), 0, vf_sem.at[m], (q_far, n))

    def vc_copy(p):
        n = 2 * p + entry(p)
        return remote(rows(v_own, 64 * p, 64), rows(vc, 64 * m, 64), 1, vc_sem.at[m], (q_peer, n))

    def vn_copy(b):
        return remote(rows(vc, 64 * b, 64), rows(vc, 64 * b, 64), 9, vn_sem.at[b], (q, beside))

    def yn_copy(p, b):
        return remote(rows(yc, 64 * b, 64), rows(yn, 64 * p, 64), 10, yn_sem.at[p], (q, beside))

    def a_copy(n):
        return remote(rows(a_send, 64 * n, 64), rows(a_recv, 64 * m, 64), 2, a_sem.at[m], (q_far, n))

    def b_copy(n):
        return remote(rows(b_send, 64 * n, 64), rows(b_recv, 64 * m, 64), 3, b_sem.at[m], (q_peer, n))

    def vr_copy(b):
        return remote(rows(vc, 64 * b + 32 * lax.rem(m, 2), 32), rows(vf, 64 * b + 32, 32), 11, vf_sem.at[b], (q_far, m))

    def vp_copy(b, off):
        return remote(rows(vf, 64 * b + 32 - off, 32), rows(vf, 64 * b + off, 32), 4, vp_sem.at[b], (q_peer, m))

    def x_copy(b, off):
        return remote(rows(yf, 64 * b + off, 32), rows(yx, 32 * b, 32), 5, x_sem.at[b], (q_peer, m))

    def yr_copy(b):
        return remote(rows(yf, 64 * b + 32, 32), rows(yr, 32 * b, 32), 12, yr_sem.at[b], (q_far, m))

    def yf_copy(b):
        return remote(rows(yf, 64 * b, 32), rows(yf_recv, 32 * m, 32), 6, yf_sem.at[m], (q_far, b))

    def yc_copy(b):
        return remote(rows(yc, 64 * b, 64), rows(yc_recv, 64 * mine, 64), 7, yc_sem.at[mine], (q_peer, b))

    peer_copy = remote(s_one, s_one_peer, 8, peer_sem, (q_peer, m))

    loads[0].wait()
    loads[1].wait()
    pl.semaphore_wait(barrier, 2 * groups + 1)
    peer_copy.start()

    def both(p):
        return (2 * p, 2 * p + 1)

    def arrived(dst, sem):
        remote(dst, dst, 0, sem, (q_peer, m)).wait_recv()

    def send_vectors(step):
        p = pair_at(step)
        vc_copy(p).start()

        @pl.when(step >= half)
        def _():
            for n in both(p):
                vf_copy(n).start()

    def make_sources(step):
        p = pair_at(step)
        mix_copy(0, p).wait()
        mix_copy(1, p).wait()
        first = [rows(s_two, 32 * n, 32)[...] for n in both(p)]
        for k, n in enumerate(both(p)):
            rows(b_send, 64 * n, 32)[...] = dot_nt(first[0], lm[n, k])
            rows(b_send, 64 * n + 32, 32)[...] = dot_nt(first[1], lm[n, 1 - k])
            rows(a_send, 64 * n, 32)[...] = dot_nt(rows(s_one, 32 * n, 32)[...], qm[n, 0])
            rows(a_send, 64 * n + 32, 32)[...] = dot_nt(rows(s_one_peer, 32 * n, 32)[...], qm[n, 1])

    def send_sources(step):
        for n in both(pair_at(step)):
            a_copy(n).start()
            b_copy(n).start()

    def make_targets(step):
        p = pair_at(step)
        mix_copy(2, p).wait()
        mix_copy(3, p).wait()
        for basis, mix, out in ((t_one, tm_one, p_one), (t_two, tm_two, p_two)):
            for k, n in enumerate(both(p)):
                t = rows(basis, 32 * n, 32)[...]
                rows(out, 128 * p + 32 * k, 32)[...] = dot(t, mix[n, k])
                rows(out, 128 * p + 64 + 32 * k, 32)[...] = dot(t, mix[n, 1 - k])

    def relay(step):
        p = pair_at(step)
        b = 2 * p + entry(p)
        arrived(rows(vc, 64 * b, 64), vc_sem.at[b])
        vn_copy(b).start()

        @pl.when(step < half)
        def _():
            vr_copy(b).start()

    def cross(step):
        p = pair_at(step)
        b = 2 * p + 1 - entry(p)
        arrived(rows(vc, 64 * b, 64), vn_sem.at[b])
        vr_copy(b).start()

    def share(step):
        off = direct_at(step)
        for b in both(pair_at(step)):
            arrived(rows(vf, 64 * b + 32 - off, 32), vf_sem.at[b])
            vp_copy(b, off).start()

    def apply(step):
        p = pair_at(step)
        off = direct_at(step)
        for b in both(p):
            arrived(rows(vf, 64 * b + off, 32), vp_sem.at[b])
            arrived(rows(a_recv, 64 * b, 64), a_sem.at[b])
            arrived(rows(b_recv, 64 * b, 64), b_sem.at[b])
        @pl.when(step >= half)
        def _():
            b = 2 * p + 1 - entry(p)
            arrived(rows(vc, 64 * b, 64), vn_sem.at[b])

        v = rows(v_own, 64 * p, 64)[...]
        box = rows(near_own, 64 * p, 64)[...]
        w = 0.5 * v + dot(box, v)
        for k, b in enumerate(both(p)):
            f = rows(p_one, 128 * p + 64 * k, 64)[...]
            c = rows(p_two, 128 * p + 64 * k, 64)[...]
            w = w + dot(dot_nt(f, rows(a_recv, 64 * b, 64)[...]), rows(vf, 64 * b, 64)[...])
            w = w + dot(dot_nt(c, rows(b_recv, 64 * b, 64)[...]), rows(vc, 64 * b, 64)[...])
        for k, b in enumerate(both(p)):
            f = rows(p_one, 128 * p + 64 * k, 64)[...]
            c = rows(p_two, 128 * p + 64 * k, 64)[...]
            rows(yf, 64 * b, 64)[...] = dot(dot_nt(rows(a_recv, 64 * b, 64)[...], f), w)
            rows(yc, 64 * b, 64)[...] = dot(dot_nt(rows(b_recv, 64 * b, 64)[...], c), w)
        rows(product, 64 * p, 64)[...] = 0.5 * w + dot_tn(box, w)

    def send_applied(step):
        p = pair_at(step)
        off = direct_at(step)
        for b in both(p):
            x_copy(b, off).start()

        @pl.when(step >= half)
        def _():
            yn_copy(p, 2 * p + 1 - entry(p)).start()

    def join(step):
        off = direct_at(step)
        for b in both(pair_at(step)):
            arrived(rows(yx, 32 * b, 32), x_sem.at[b])
            rows(yf, 64 * b + 32 - off, 32)[...] += rows(yx, 32 * b, 32)[...]

    def send_joined(step):
        p = pair_at(step)

        @pl.when(step < half)
        def _():
            for b in both(p):
                yr_copy(b).start()

        @pl.when(step >= half)
        def _():
            for b in both(p):
                yf_copy(b).start()

    def add(step):
        for b in both(pair_at(step)):
            arrived(rows(yr, 32 * b, 32), yr_sem.at[b])
            rows(yc, 64 * b + 32 * lax.rem(m, 2), 32)[...] += rows(yr, 32 * b, 32)[...]

    def send_added(step):
        p = pair_at(step)
        yn_copy(p, 2 * p + 1 - entry(p)).start()

    def gather(step):
        p = pair_at(step)
        b = 2 * p + entry(p)
        arrived(rows(yn, 64 * p, 64), yn_sem.at[p])
        rows(yc, 64 * b, 64)[...] += rows(yn, 64 * p, 64)[...]

    def send_gathered(step):
        p = pair_at(step)
        yc_copy(2 * p + entry(p)).start()

    def staged(step, stage, lag, first, last):
        @pl.when((step >= first + lag) & (step < last + lag))
        def _():
            stage(step - lag)

    def staggered(step, name, *stages):
        for stage in stages:
            if name in RELAYED:
                staged(step, stage, RELAYED[name], 0, half)
            if name in STRAIGHT:
                staged(step, stage, STRAIGHT[name], half, pairs)

    for step in range(AHEAD):
        send_vectors(step)
    for copy in loads[2:]:
        copy.wait()
    for k in range(near_own.shape[0] // 128):
        near_own[pl.ds(128 * k, 128)] = near_flat[:, pl.ds(128 * k, 128)].T
    peer_copy.wait()

    def stream(step, carry):
        @pl.when(step < pairs - AHEAD)
        def _():
            send_vectors(step + AHEAD)

        staged(step, make_sources, 0, 0, pairs)
        staggered(step, "relay", relay)
        staggered(step, "cross", cross)
        staggered(step, "share", share)
        staged(step, send_sources, 0, 0, pairs)
        staggered(step, "gather", gather)
        staggered(step, "add", add)
        staggered(step, "join", join)
        staggered(step, "gather", send_gathered)
        staggered(step, "add", send_added)
        staggered(step, "join", send_joined)
        staggered(step, "target", make_targets)
        staggered(step, "apply", apply)
        staggered(step, "apply", send_applied)
        return carry

    lax.fori_loop(0, half + max(RELAYED["gather"], half + STRAIGHT["gather"]), stream, 0)

    def finish(step, carry):
        p = pair_at(step)
        arrived(rows(yc_recv, 64 * p, 64), yc_sem.at[p])
        rows(product, 64 * p, 64)[...] += rows(yc_recv, 64 * p, 64)[...]

        @pl.when(step >= half)
        def _():
            for b in both(p):
                arrived(rows(yf_recv, 32 * b, 32), yf_sem.at[b])
            rows(product, 64 * p, 64)[...] += rows(yf_recv, 64 * p, 64)[...]

        return carry

    lax.fori_loop(0, pairs, finish, 0)

    whole, part = v_own, rows(v_own, 0, 16 * groups)
    for k, ref in (
        (0, part),
        (1, whole),
        (2, a_send),
        (3, b_send),
        (4, whole),
        (5, whole),
        (6, part),
        (7, whole),
        (9, whole),
        (10, whole),
        (11, part),
        (12, part),
    ):
        remote(ref, ref, k, peer_sem, (q_peer, m)).wait_send()


def body(sketch, near_field, source_one, source_two, target_one, target_two, quarter_mix, leaf_mix, mix_one, mix_two):
    groups = lax.axis_size("blk")
    local, vectors = sketch.shape
    rank = source_one.shape[1]
    any_space = pl.BlockSpec(memory_space=pl.ANY)
    basis = pltpu.VMEM((local, rank), F32)
    mixes = pltpu.VMEM(quarter_mix.shape, F32)
    single = pltpu.VMEM((local, vectors), F32)
    double = pltpu.VMEM((2 * local, vectors), F32)
    nodes = pltpu.VMEM((2 * local, rank), F32)
    dma = pltpu.SemaphoreType.DMA


    return pl.pallas_call(
        functools.partial(kernel, groups),
        out_shape=jax.ShapeDtypeStruct((local, vectors), F32),
        in_specs=[any_space] * 10,
        out_specs=pl.BlockSpec(memory_space=pltpu.VMEM),
        scratch_shapes=[
            single,
            pltpu.VMEM(near_field.shape[::-1], F32),
            pltpu.VMEM(near_field.shape, F32),
            basis,
            basis,
            basis,
            basis,
            basis,
            mixes,
            mixes,
            mixes,
            mixes,
            nodes,
            nodes,
            nodes,
            nodes,
            double,
            double,
            nodes,
            nodes,
            double,
            single,
            double,
            single,
            single,
            single,
            single,
            dma((6,)),
            dma((4, groups // 2)),
            dma(()),
            dma((13,)),
            dma((groups,)),
            dma((groups,)),
            dma((groups,)),
            dma((groups,)),
            dma((groups,)),
            dma((groups,)),
            dma((groups,)),
            dma((groups // 2,)),
            dma((groups,)),
            dma((groups,)),
            dma((groups // 2,)),
        ],
        compiler_params=pltpu.CompilerParams(
            collective_id=0, has_side_effects=True, vmem_limit_bytes=60 * 1024 * 1024
        ),
    )(sketch, near_field.T, source_one, source_two, target_one, target_two, quarter_mix, leaf_mix, mix_one, mix_two)


def solution(mesh):
    rows_split = P(("half", "blk"), None)
    nodes_split = P(("half", "blk"), None, None, None)
    return jax.shard_map(
        body,
        mesh=mesh,
        in_specs=(rows_split,) * 6 + (nodes_split,) * 4,
        out_specs=rows_split,
        check_vma=False,
    )
```

```python
import functools

import jax
import jax.numpy as jnp
from jax import lax
from jax.experimental import pallas as pl
from jax.experimental.pallas import tpu as pltpu
from jax.sharding import PartitionSpec as P

MESH = pl.DeviceIdType.MESH
HIGH = lax.Precision.HIGHEST
F32 = jnp.float32


def dot(a, b):
    return lax.dot_general(a, b, (((1,), (0,)), ((), ())), precision=HIGH, preferred_element_type=F32)


def dot_nt(a, b):
    return lax.dot_general(a, b, (((1,), (1,)), ((), ())), precision=HIGH, preferred_element_type=F32)


def dot_tn(a, b):
    return lax.dot_general(a, b, (((0,), (0,)), ((), ())), precision=HIGH, preferred_element_type=F32)


def xor(a, b, bits):
    total = 0
    for k in range(bits):
        w = 1 << k
        total = total + lax.rem(lax.div(a, w) + lax.div(b, w), 2) * w
    return total


def reversed_bits(a, bits):
    total = 0
    for k in range(bits):
        total = total + lax.rem(lax.div(a, 1 << k), 2) * (1 << (bits - 1 - k))
    return total


RELAYED = dict(relay=1, cross=2, share=3, target=3, apply=4, join=5, add=6, gather=7)
STRAIGHT = dict(relay=1, share=1, target=1, apply=2, join=3, gather=4)
AHEAD = 2


def rows(ref, start, count):
    return ref.at[pl.ds(pl.multiple_of(start, 32), count)]


def kernel(
    groups,
    sketch,
    near,
    source_one,
    source_two,
    target_one,
    target_two,
    quarter_mix,
    leaf_mix,
    target_mix_one,
    target_mix_two,
    product,
    v_own,
    near_flat,
    near_own,
    s_one,
    s_one_peer,
    s_two,
    t_one,
    t_two,
    qm,
    lm,
    tm_one,
    tm_two,
    a_send,
    b_send,
    a_recv,
    b_recv,
    vf,
    vc,
    p_one,
    p_two,
    yf,
    yx,
    yc,
    yn,
    yr,
    yf_recv,
    yc_recv,
    load_sem,
    mix_sem,
    peer_sem,
    send_sem,
    vf_sem,
    vp_sem,
    vc_sem,
    vn_sem,
    a_sem,
    b_sem,
    x_sem,
    yn_sem,
    yr_sem,
    yf_sem,
    yc_sem,
):
    pairs = groups // 2
    half = pairs // 2
    bits = pairs.bit_length() - 1
    q = lax.axis_index("half")
    m = lax.axis_index("blk")
    mine = lax.div(m, 2)
    q_peer = xor(q, 1, 2)
    q_far = xor(q, 2, 2)
    beside = xor(m, 1, 1) + 2 * mine

    def pair_at(step):
        inner = reversed_bits(lax.rem(step, half), bits - 1)
        inner = inner + lax.div(step, half) * (half - 1 - 2 * inner)
        return xor(mine, inner + inner - lax.rem(inner, 2) + 2 * lax.div(step, half), bits)

    def direct_at(step):
        return lax.div(step, half) * 32

    def entry(p):
        return lax.rem(m + mine + p, 2)

    barrier = pltpu.get_barrier_semaphore()

    def greet(n, carry):
        pl.semaphore_signal(barrier, inc=1, device_id=(q_far, n), device_id_type=MESH)
        pl.semaphore_signal(barrier, inc=1, device_id=(q_peer, n), device_id_type=MESH)
        return carry

    lax.fori_loop(0, groups, greet, 0)
    pl.semaphore_signal(barrier, inc=1, device_id=(q, beside), device_id_type=MESH)

    loads = [
        pltpu.make_async_copy(src, dst, load_sem.at[k])
        for k, (src, dst) in enumerate(
            (
                (sketch, v_own),
                (source_one, s_one),
                (source_two, s_two),
                (target_one, t_one),
                (target_two, t_two),
                (near, near_flat),
            )
        )
    ]
    for copy in loads:
        copy.start()

    def mix_copy(k, p):
        src, dst = ((quarter_mix, qm), (leaf_mix, lm), (target_mix_one, tm_one), (target_mix_two, tm_two))[k]
        here = pl.ds(2 * p, 2)
        return pltpu.make_async_copy(src.at[here], dst.at[here], mix_sem.at[k, p])

    def load_source_mix(step, carry):
        p = pair_at(step)
        mix_copy(0, p).start()
        mix_copy(1, p).start()
        return carry

    def load_target_mix(step, carry):
        p = pair_at(step)
        mix_copy(2, p).start()
        mix_copy(3, p).start()
        return carry

    lax.fori_loop(0, pairs, load_source_mix, 0)
    lax.fori_loop(0, pairs, load_target_mix, 0)

    def remote(src, dst, k, recv, to):
        return pltpu.make_async_remote_copy(
            src_ref=src, dst_ref=dst, send_sem=send_sem.at[k], recv_sem=recv, device_id=to, device_id_type=MESH
        )

    def vf_copy(n):
        return remote(rows(v_own, 32 * n, 32), rows(vf, 64 * m, 32), 0, vf_sem.at[m], (q_far, n))

    def vc_copy(p):
        n = 2 * p + entry(p)
        return remote(rows(v_own, 64 * p, 64), rows(vc, 64 * m, 64), 1, vc_sem.at[m], (q_peer, n))

    def vn_copy(b):
        return remote(rows(vc, 64 * b, 64), rows(vc, 64 * b, 64), 9, vn_sem.at[b], (q, beside))

    def yn_copy(p, b):
        return remote(rows(yc, 64 * b, 64), rows(yn, 64 * p, 64), 10, yn_sem.at[p], (q, beside))

    def a_copy(n):
        return remote(rows(a_send, 64 * n, 64), rows(a_recv, 64 * m, 64), 2, a_sem.at[m], (q_far, n))

    def b_copy(n):
        return remote(rows(b_send, 64 * n, 64), rows(b_recv, 64 * m, 64), 3, b_sem.at[m], (q_peer, n))

    def vr_copy(b):
        return remote(rows(vc, 64 * b + 32 * lax.rem(m, 2), 32), rows(vf, 64 * b + 32, 32), 11, vf_sem.at[b], (q_far, m))

    def vp_copy(b, off):
        return remote(rows(vf, 64 * b + 32 - off, 32), rows(vf, 64 * b + off, 32), 4, vp_sem.at[b], (q_peer, m))

    def x_copy(b, off):
        return remote(rows(yf, 64 * b + off, 32), rows(yx, 32 * b, 32), 5, x_sem.at[b], (q_peer, m))

    def yr_copy(b):
        return remote(rows(yf, 64 * b + 32, 32), rows(yr, 32 * b, 32), 12, yr_sem.at[b], (q_far, m))

    def yf_copy(b):
        return remote(rows(yf, 64 * b, 32), rows(yf_recv, 32 * m, 32), 6, yf_sem.at[m], (q_far, b))

    def yc_copy(b):
        return remote(rows(yc, 64 * b, 64), rows(yc_recv, 64 * mine, 64), 7, yc_sem.at[mine], (q_peer, b))

    peer_copy = remote(s_one, s_one_peer, 8, peer_sem, (q_peer, m))

    loads[0].wait()
    loads[1].wait()
    pl.semaphore_wait(barrier, 2 * groups + 1)
    peer_copy.start()

    def both(p):
        return (2 * p, 2 * p + 1)

    def arrived(dst, sem):
        remote(dst, dst, 0, sem, (q_peer, m)).wait_recv()

    def send_vectors(step):
        p = pair_at(step)
        vc_copy(p).start()

        @pl.when(step >= half)
        def _():
            for n in both(p):
                vf_copy(n).start()

    def make_sources(step):
        p = pair_at(step)
        mix_copy(0, p).wait()
        mix_copy(1, p).wait()
        first = [rows(s_two, 32 * n, 32)[...] for n in both(p)]
        for k, n in enumerate(both(p)):
            rows(b_send, 64 * n, 32)[...] = dot_nt(first[0], lm[n, k])
            rows(b_send, 64 * n + 32, 32)[...] = dot_nt(first[1], lm[n, 1 - k])
            rows(a_send, 64 * n, 32)[...] = dot_nt(rows(s_one, 32 * n, 32)[...], qm[n, 0])
            rows(a_send, 64 * n + 32, 32)[...] = dot_nt(rows(s_one_peer, 32 * n, 32)[...], qm[n, 1])

    def send_sources(step):
        for n in both(pair_at(step)):
            a_copy(n).start()
            b_copy(n).start()

    def make_targets(step):
        p = pair_at(step)
        mix_copy(2, p).wait()
        mix_copy(3, p).wait()
        for basis, mix, out in ((t_one, tm_one, p_one), (t_two, tm_two, p_two)):
            for k, n in enumerate(both(p)):
                t = rows(basis, 32 * n, 32)[...]
                rows(out, 128 * p + 32 * k, 32)[...] = dot(t, mix[n, k])
                rows(out, 128 * p + 64 + 32 * k, 32)[...] = dot(t, mix[n, 1 - k])

    def relay(step):
        p = pair_at(step)
        b = 2 * p + entry(p)
        arrived(rows(vc, 64 * b, 64), vc_sem.at[b])
        vn_copy(b).start()

        @pl.when(step < half)
        def _():
            vr_copy(b).start()

    def cross(step):
        p = pair_at(step)
        b = 2 * p + 1 - entry(p)
        arrived(rows(vc, 64 * b, 64), vn_sem.at[b])
        vr_copy(b).start()

    def share(step):
        off = direct_at(step)
        for b in both(pair_at(step)):
            arrived(rows(vf, 64 * b + 32 - off, 32), vf_sem.at[b])
            vp_copy(b, off).start()

    def apply(step):
        p = pair_at(step)
        off = direct_at(step)
        for b in both(p):
            arrived(rows(vf, 64 * b + off, 32), vp_sem.at[b])
            arrived(rows(a_recv, 64 * b, 64), a_sem.at[b])
            arrived(rows(b_recv, 64 * b, 64), b_sem.at[b])
        @pl.when(step >= half)
        def _():
            b = 2 * p + 1 - entry(p)
            arrived(rows(vc, 64 * b, 64), vn_sem.at[b])

        v = rows(v_own, 64 * p, 64)[...]
        box = rows(near_own, 64 * p, 64)[...]
        w = 0.5 * v + dot(box, v)
        for k, b in enumerate(both(p)):
            f = rows(p_one, 128 * p + 64 * k, 64)[...]
            c = rows(p_two, 128 * p + 64 * k, 64)[...]
            w = w + dot(dot_nt(f, rows(a_recv, 64 * b, 64)[...]), rows(vf, 64 * b, 64)[...])
            w = w + dot(dot_nt(c, rows(b_recv, 64 * b, 64)[...]), rows(vc, 64 * b, 64)[...])
        for k, b in enumerate(both(p)):
            f = rows(p_one, 128 * p + 64 * k, 64)[...]
            c = rows(p_two, 128 * p + 64 * k, 64)[...]
            rows(yf, 64 * b, 64)[...] = dot(dot_nt(rows(a_recv, 64 * b, 64)[...], f), w)
            rows(yc, 64 * b, 64)[...] = dot(dot_nt(rows(b_recv, 64 * b, 64)[...], c), w)
        rows(product, 64 * p, 64)[...] = 0.5 * w + dot_tn(box, w)

    def send_applied(step):
        p = pair_at(step)
        off = direct_at(step)
        for b in both(p):
            x_copy(b, off).start()

        @pl.when(step >= half)
        def _():
            yn_copy(p, 2 * p + 1 - entry(p)).start()

    def join(step):
        off = direct_at(step)
        for b in both(pair_at(step)):
            arrived(rows(yx, 32 * b, 32), x_sem.at[b])
            rows(yf, 64 * b + 32 - off, 32)[...] += rows(yx, 32 * b, 32)[...]

    def send_joined(step):
        p = pair_at(step)

        @pl.when(step < half)
        def _():
            for b in both(p):
                yr_copy(b).start()

        @pl.when(step >= half)
        def _():
            for b in both(p):
                yf_copy(b).start()

    def add(step):
        for b in both(pair_at(step)):
            arrived(rows(yr, 32 * b, 32), yr_sem.at[b])
            rows(yc, 64 * b + 32 * lax.rem(m, 2), 32)[...] += rows(yr, 32 * b, 32)[...]

    def send_added(step):
        p = pair_at(step)
        yn_copy(p, 2 * p + 1 - entry(p)).start()

    def gather(step):
        p = pair_at(step)
        b = 2 * p + entry(p)
        arrived(rows(yn, 64 * p, 64), yn_sem.at[p])
        rows(yc, 64 * b, 64)[...] += rows(yn, 64 * p, 64)[...]

    def send_gathered(step):
        p = pair_at(step)
        yc_copy(2 * p + entry(p)).start()

    def staged(step, stage, lag, first, last):
        @pl.when((step >= first + lag) & (step < last + lag))
        def _():
            stage(step - lag)

    def staggered(step, name, *stages):
        for stage in stages:
            if name in RELAYED:
                staged(step, stage, RELAYED[name], 0, half)
            if name in STRAIGHT:
                staged(step, stage, STRAIGHT[name], half, pairs)

    for step in range(AHEAD):
        send_vectors(step)
    for copy in loads[2:]:
        copy.wait()
    for k in range(near_own.shape[0] // 128):
        near_own[pl.ds(128 * k, 128)] = near_flat[:, pl.ds(128 * k, 128)].T
    peer_copy.wait()

    def stream(step, carry):
        @pl.when(step < pairs - AHEAD)
        def _():
            send_vectors(step + AHEAD)

        staggered(step, "relay", relay)
        staggered(step, "cross", cross)
        staggered(step, "share", share)
        staged(step, make_sources, 0, 0, pairs)
        staged(step, send_sources, 0, 0, pairs)
        staggered(step, "gather", gather)
        staggered(step, "add", add)
        staggered(step, "join", join)
        staggered(step, "gather", send_gathered)
        staggered(step, "add", send_added)
        staggered(step, "join", send_joined)
        staggered(step, "target", make_targets)
        staggered(step, "apply", apply)
        staggered(step, "apply", send_applied)
        return carry

    lax.fori_loop(0, half + max(RELAYED["gather"], half + STRAIGHT["gather"]), stream, 0)

    def finish(step, carry):
        p = pair_at(step)
        arrived(rows(yc_recv, 64 * p, 64), yc_sem.at[p])
        rows(product, 64 * p, 64)[...] += rows(yc_recv, 64 * p, 64)[...]

        @pl.when(step >= half)
        def _():
            for b in both(p):
                arrived(rows(yf_recv, 32 * b, 32), yf_sem.at[b])
            rows(product, 64 * p, 64)[...] += rows(yf_recv, 64 * p, 64)[...]

        return carry

    lax.fori_loop(0, pairs, finish, 0)

    whole, part = v_own, rows(v_own, 0, 16 * groups)
    for k, ref in (
        (0, part),
        (1, whole),
        (2, a_send),
        (3, b_send),
        (4, whole),
        (5, whole),
        (6, part),
        (7, whole),
        (9, whole),
        (10, whole),
        (11, part),
        (12, part),
    ):
        remote(ref, ref, k, peer_sem, (q_peer, m)).wait_send()


def body(sketch, near_field, source_one, source_two, target_one, target_two, quarter_mix, leaf_mix, mix_one, mix_two):
    groups = lax.axis_size("blk")
    local, vectors = sketch.shape
    rank = source_one.shape[1]
    any_space = pl.BlockSpec(memory_space=pl.ANY)
    basis = pltpu.VMEM((local, rank), F32)
    mixes = pltpu.VMEM(quarter_mix.shape, F32)
    single = pltpu.VMEM((local, vectors), F32)
    double = pltpu.VMEM((2 * local, vectors), F32)
    nodes = pltpu.VMEM((2 * local, rank), F32)
    dma = pltpu.SemaphoreType.DMA


    return pl.pallas_call(
        functools.partial(kernel, groups),
        out_shape=jax.ShapeDtypeStruct((local, vectors), F32),
        in_specs=[any_space] * 10,
        out_specs=pl.BlockSpec(memory_space=pltpu.VMEM),
        scratch_shapes=[
            single,
            pltpu.VMEM(near_field.shape[::-1], F32),
            pltpu.VMEM(near_field.shape, F32),
            basis,
            basis,
            basis,
            basis,
            basis,
            mixes,
            mixes,
            mixes,
            mixes,
            nodes,
            nodes,
            nodes,
            nodes,
            double,
            double,
            nodes,
            nodes,
            double,
            single,
            double,
            single,
            single,
            single,
            single,
            dma((6,)),
            dma((4, groups // 2)),
            dma(()),
            dma((13,)),
            dma((groups,)),
            dma((groups,)),
            dma((groups,)),
            dma((groups,)),
            dma((groups,)),
            dma((groups,)),
            dma((groups,)),
            dma((groups // 2,)),
            dma((groups,)),
            dma((groups,)),
            dma((groups // 2,)),
        ],
        compiler_params=pltpu.CompilerParams(
            collective_id=0, has_side_effects=True, vmem_limit_bytes=60 * 1024 * 1024
        ),
    )(sketch, near_field.T, source_one, source_two, target_one, target_two, quarter_mix, leaf_mix, mix_one, mix_two)


def solution(mesh):
    rows_split = P(("half", "blk"), None)
    nodes_split = P(("half", "blk"), None, None, None)
    return jax.shard_map(
        body,
        mesh=mesh,
        in_specs=(rows_split,) * 6 + (nodes_split,) * 4,
        out_specs=rows_split,
        check_vma=False,
    )
```
